32 devices in a mesh: ma: 8 (over z, x), lev: 4 (over y, core).
Axes of the slice: x: 2, y: 2, z: 4, core: 2. Of those that a mesh axis runs over, the one named last changes fastest.
Arguments:
- forcing: float32 [72, 2, 1280, 1280], P('lev', None, 'ma'), may hold values from -80 to 80
- coupling: float32 [4, 1280, 1280], P(None, 'ma'), may hold values from -0.3 to 0.3
- helmholtz: float32 [1280], replicated, may hold values from 0.5 to 5
- vertical: float32 [72, 72], replicated, may hold values from -1 to 3, as said below
Outputs:
- solution: float32 [72, 2, 1280, 1280], P('lev', None, 'ma')
- norms: float32 [2], replicated
The draws below stay inside these ranges and needn't reach their ends.
Inputs may be any that keep to these rules, and one draw needn't show every extreme that they name: `vertical`: the diagonal entries lie between 1 and 3.
All inputs are finite; a program needn't handle non-finite values.
Results may differ from the reference program's by a relative error of at most 0.000071.
Values sent between devices are 32-bit elements; how exact they have to be, the bound alone decides.
A program may use at most 704 MiB of HBM per device.

```python
import math
import jax
import jax.numpy as jnp
from jax import lax

LEV = 72
WAVES = 1280
N_MA = 8


def draw_forcing(key, part):
    base_key, row_key, col_key = jax.random.split(jax.random.fold_in(key, 11), 3)
    shape = (LEV, 2, WAVES, WAVES)
    rows = jnp.arange(WAVES, dtype=jnp.float32)
    ramp = 1.0 + rows / WAVES
    spread = jnp.exp(jax.random.uniform(row_key, (WAVES,), jnp.float32, math.log(0.25), math.log(2.5)))
    columns = jnp.exp(jax.random.uniform(col_key, (WAVES,), jnp.float32, math.log(0.3), math.log(3.0)))
    base = jax.random.truncated_normal(base_key, -4.0, 4.0, shape, jnp.float32)
    return base * (ramp * spread)[None, None, :, None] * columns[None, None, None, :]


def draw_vertical(key, part):
    diag_key, off_key = jax.random.split(jax.random.fold_in(key, 23), 2)
    diagonal = jax.random.uniform(diag_key, (LEV,), jnp.float32, 1.0, 3.0)
    offdiag = jax.random.truncated_normal(off_key, -4.0, 4.0, (LEV, LEV), jnp.float32) / LEV
    identity = jnp.eye(LEV, dtype=jnp.float32)
    return offdiag * (1.0 - identity) + diagonal[None, :] * identity


def block_scale(own_key, shape, cuts, low, largest):
    level, own = 1.0, jax.random.fold_in(own_key, 6)
    for position, shards_of in cuts:
        steps = jnp.exp(jax.random.uniform(jax.random.fold_in(own, position), (shards_of,), jnp.float32, low / len(cuts), largest / len(cuts)))
        level = level * jnp.repeat(steps, shape[position] // shards_of).reshape([-1 if axis == position else 1 for axis in range(len(shape))])
    return level


def setup_inputs(seed: int = 0) -> dict:
    seeds = jax.random.split(jax.random.key(seed), 5)
    return {
        "forcing": draw_forcing(jax.random.fold_in(seeds[4], 71), 0),
        "coupling": jnp.clip(jax.random.uniform(seeds[1], (4, WAVES, WAVES), jnp.float32, -0.3, 0.3) * block_scale(seeds[1], (4, WAVES, WAVES), ((1, 8),), -0.4, 0.0), -0.3, 0.3),
        "helmholtz": jnp.clip(jnp.exp(jax.random.uniform(seeds[2], (WAVES,), jnp.float32, math.log(0.5), math.log(5.0))), 0.5, 5.0),
        "vertical": draw_vertical(jax.random.fold_in(seeds[4], 71), 0),
    }


OFFSETS = (-2, -1, 1, 2)

def storage_waves():
    per_owner = WAVES // N_MA
    place = jnp.arange(WAVES, dtype=jnp.int32)
    owner = place // per_owner
    fold = place % per_owner
    return fold * N_MA + jnp.where(fold % 2 == 0, owner, N_MA - 1 - owner)

def reference(forcing, coupling, helmholtz, vertical):
    waves = storage_waves()
    row_of_wave = jnp.argsort(waves).astype(jnp.int32)
    positions = jnp.arange(WAVES, dtype=jnp.int32)
    live = (positions[None, :] >= waves[:, None]).astype(jnp.float32)[None, None]
    scale = 1.0 / (1.0 + helmholtz[None, :] * jnp.diagonal(vertical)[:, None])
    scale = scale[:, None, None, :]

    def operator(values):
        mixed = jnp.einsum('kl,lcin->kcin', vertical, values, precision=lax.Precision.HIGHEST)
        result = values + helmholtz[None, None, None, :] * mixed
        for place, offset in enumerate(OFFSETS):
            target = waves + offset
            valid = ((target >= 0) & (target < WAVES)).astype(jnp.float32)
            source = row_of_wave[jnp.clip(target, 0, WAVES - 1)].astype(jnp.int32)
            moved = jnp.take(values, source, axis=2) * valid[None, None, :, None]
            result = result + coupling[place][None, None] * moved
        return result * live
    rhs = forcing * live
    first = scale * rhs
    residual = rhs - operator(first)
    solution = first + scale * residual
    count = LEV * WAVES * (WAVES + 1)
    sums = jnp.stack([jnp.sum(rhs * rhs), jnp.sum(residual * residual)])
    norms = jnp.sqrt(sums / count)
    return (solution, norms)
```

```python
import jax
import jax.numpy as jnp
from jax import lax
from jax.sharding import PartitionSpec as P

OFFSETS = (-2, -1, 1, 2)
COLUMN_STEP = 256


def shifted(block, axis, distance):
    devices = range(lax.axis_size(axis))
    route = [(i - distance, i) for i in devices if i - distance in devices]
    return lax.ppermute(block, axis, route)


def swapped(block, axis):
    return lax.ppermute(block, axis, [(i, i ^ 1) for i in range(lax.axis_size(axis))])


def owned_waves(rows, owners, index):
    fold = jnp.arange(rows, dtype=jnp.int32)
    return fold * owners + jnp.where(fold % 2 == 0, index, owners - 1 - index)


def coupling_weights(coupling, rows, owners, target, holder):
    fold = jnp.arange(rows, dtype=jnp.int32)
    waves = owned_waves(rows, owners, target)
    totals = [0.0] * 5
    for place, offset in enumerate(OFFSETS):
        wave = waves + offset
        valid = (wave >= 0) & (wave < rows * owners)
        wave = jnp.clip(wave, 0, rows * owners - 1)
        source_fold = wave // owners
        position = wave % owners
        owner = jnp.where(source_fold % 2 == 0, position, owners - 1 - position)
        delta = source_fold - fold
        own = valid & (owner == holder)
        level = valid & (delta == 0)
        picks = (
            own & (delta == -1),
            own & (delta == 0),
            own & (delta == 1),
            level & (owner == holder - 2),
            level & (owner == holder + 2),
        )
        for kind, pick in enumerate(picks):
            totals[kind] = totals[kind] + coupling[place] * pick.astype(jnp.float32)[:, None]
    return totals


def body(forcing, coupling, helmholtz, vertical):
    owners = lax.axis_size("ma")
    index = lax.axis_index("ma")
    partner = index + 1 - 2 * (index % 2)
    levels, _, rows, width = forcing.shape
    all_levels = levels * lax.axis_size("lev")
    start = lax.axis_index("lev") * levels
    weights = lax.dynamic_slice_in_dim(vertical, start, levels, 0)
    diagonal = lax.dynamic_slice_in_dim(jnp.diagonal(vertical), start, levels, 0)
    waves = owned_waves(rows, owners, index)
    positions = jnp.arange(width, dtype=jnp.int32)
    live = (positions[None, :] >= waves[:, None]).astype(jnp.float32)
    scale = 1.0 / (1.0 + helmholtz[None, :] * diagonal[:, None])

    mine = coupling_weights(coupling, rows, owners, index, index)
    theirs = coupling_weights(swapped(coupling, "ma"), rows, owners, partner, index)
    mine = lax.optimization_barrier(jnp.stack(mine))
    theirs = lax.optimization_barrier(jnp.stack(theirs))

    groups = max(width // COLUMN_STEP, 1)
    if width % COLUMN_STEP or rows % groups:
        groups = 1
    size = rows // groups
    solution = jnp.zeros_like(forcing)
    first_sum = jnp.float32(0)
    second_sum = jnp.float32(0)
    sent = []
    for group in range(groups):
        low, left = group * size, group * size * owners
        rhs = forcing[:, :, low : low + size, left:] * live[low : low + size, left:]
        first = lax.optimization_barrier(scale[:, None, None, left:] * rhs)
        below = shifted(first, "ma", 2)
        above = shifted(first, "ma", -2)
        gathered = lax.all_gather(first, "lev", axis=0, tiled=True)
        sent.append((first, below, above, gathered))
    for group in range(groups):
        low, left = group * size, group * size * owners
        first, below, above, gathered = sent[group]
        mask = live[low : low + size, left:]
        rhs = forcing[:, :, low : low + size, left:] * mask
        column_scale = scale[:, None, None, left:]
        empty = jnp.zeros_like(first[:, :, :1])
        before, after = empty, empty
        if group > 0:
            before = sent[group - 1][0][:, :, -1:, size * owners :]
        if group < groups - 1:
            gap = ((0, 0), (0, 0), (0, 0), (size * owners, 0))
            after = jnp.pad(sent[group + 1][0][:, :, :1], gap)
        down = jnp.concatenate([before, first[:, :, :-1]], axis=2)
        up = jnp.concatenate([first[:, :, 1:], after], axis=2)
        fields = (down, first, up, below, above)

        def combined(table):
            part = table[:, low : low + size, left:]
            return sum(part[kind][None, None] * field for kind, field in enumerate(fields))

        received = swapped(combined(theirs), "ma")
        mixed = jnp.einsum("kl,lcin->kcin", weights, gathered, precision=lax.Precision.HIGH)
        result = first + helmholtz[None, None, None, left:] * mixed
        result = result + combined(mine) + received
        residual = rhs - result * mask
        first_sum = first_sum + jnp.sum(rhs * rhs)
        second_sum = second_sum + jnp.sum(residual * residual)
        update = first + column_scale * residual
        solution = lax.dynamic_update_slice(solution, update, (0, 0, low, left))
    sums = lax.psum(jnp.stack([first_sum, second_sum]), ("ma", "lev"))
    norms = jnp.sqrt(sums / (all_levels * width * (width + 1)))
    return (solution, norms)


def solution(mesh):
    in_specs = (P("lev", None, "ma", None), P(None, "ma", None), P(), P())
    out_specs = (P("lev", None, "ma", None), P())
    return jax.shard_map(body, mesh=mesh, in_specs=in_specs, out_specs=out_specs, check_vma=False)
```
